32 devices in a mesh: grp: 4 (over y, core), dev: 8 (over z, x).
Axes of the slice: x: 2, y: 2, z: 4, core: 2. Of those that a mesh axis runs over, the one named last changes fastest.
Arguments:
- interior_stiffness: float32 [64, 8, 128, 128], P(('grp', 'dev')), may hold values from -6 to 8, as said below
- interior_links: float32 [64, 7, 128, 128], P(('grp', 'dev')), may hold values from -4 to 4
- coupling_stiffness: float32 [64, 128, 256], P(('grp', 'dev')), may hold values from -0.5 to 0.5
- interface_stiffness: float32 [64, 256, 256], P(('grp', 'dev')), may hold values from -5 to 5, as said below
- interior_mass: float32 [64, 1024], P(('grp', 'dev')), may hold values from 0.03 to 0.5
- interface_mass: float32 [64, 256], P(('grp', 'dev')), may hold values from 0.5 to 4
- interior_modes: float32 [64, 1024, 256], P(('grp', 'dev')), may hold values from -6 to 6
- interior_blocks: int32 [64], P(('grp', 'dev')), may hold values from 2 to 8
- interface_blocks: int32 [64, 2], P(('grp', 'dev')), may hold values from 0 to 7, as said below
- parent_modes: float32 [1024, 256], P(('grp', 'dev')), may hold values from -2 to 2
Outputs:
- parent_stiffness: float32 [1024, 1024], P(('grp', 'dev'))
- parent_mass: float32 [1024, 1024], P(('grp', 'dev'))
- coupling: float32 [64, 256, 256], P(('grp', 'dev'))
- modal_stiffness: float32 [256, 256], replicated
- modal_mass: float32 [256, 256], replicated
The draws below stay inside these ranges and needn't reach their ends.
Inputs may be any that keep to these rules, and one draw needn't show every extreme that they name: `interior_stiffness`: each diagonal block is symmetric; with interior_links, the leading k blocks of every component's block-tridiagonal interior stiffness form a symmetric positive definite matrix for every k from 1 to 8. `interface_stiffness`: Symmetric. `interface_blocks`: the 2 parent blocks of one component are distinct.
All inputs are finite; a program needn't handle non-finite values.
Results may differ from the reference program's by a relative error of at most 0.0003.
Values sent between devices are 32-bit elements; how exact they have to be, the bound alone decides.
No kernel may reach another device: no remote copies, remote signals or barrier semaphores. Data moves between devices by JAX's collectives and lax.ppermute only.
A program may use at most 64 MiB of HBM per device.

```python
import math
import jax
import jax.numpy as jnp
from jax import lax

BLOCK = 128
MAXB = 8
NBB = 2
MODES = 256
PB = 8
COMPONENTS = 64
MAXI = 1024
NB = 256
NP = 1024


def chain_blocks(key):
    first_key, second_key = jax.random.split(jax.random.fold_in(key, 21))
    shape = (COMPONENTS, MAXB, BLOCK, BLOCK)
    noise_upper = jnp.clip(jax.random.normal(first_key, shape, jnp.float32), -4.0, 4.0)
    noise_lower = jnp.clip(jax.random.normal(second_key, shape, jnp.float32), -4.0, 4.0)
    shift = 0.05
    identity = jnp.eye(BLOCK, dtype=jnp.float32)
    spread = 0.35 / BLOCK ** 0.5
    upper_part = identity + spread * noise_upper
    lower_part = -0.9 * identity + spread * noise_lower
    diagonal = jnp.einsum('cikr,cikq->cirq', upper_part, upper_part) + jnp.einsum('cikr,cikq->cirq', lower_part, lower_part) + shift * identity
    diagonal = 0.5 * (diagonal + jnp.swapaxes(diagonal, 2, 3))
    links = jnp.einsum('cikr,cikq->cirq', upper_part[:, 1:], lower_part[:, :-1])
    return (diagonal, links)


def draw_interior_stiffness(key, part):
    return chain_blocks(key)[0]


def draw_interior_links(key, part):
    return chain_blocks(key)[1]


def symmetric_part(key, count, size_along):
    noise = jnp.clip(jax.random.normal(key, (count, size_along, size_along), jnp.float32), -5.0, 5.0)
    return (noise + jnp.swapaxes(noise, 1, 2)) / (2.0 * size_along) ** 0.5


def draw_interface_stiffness(key, part):
    first_key, second_key = jax.random.split(jax.random.fold_in(key, 13))
    diagonal = jnp.clip(jax.random.normal(second_key, (COMPONENTS, NB), jnp.float32), -3.0, 3.0)
    return symmetric_part(first_key, COMPONENTS, NB) + diagonal[:, :, None] * jnp.eye(NB, dtype=jnp.float32)


def draw_interface_blocks(key, part):
    member_keys = jax.random.split(jax.random.fold_in(key, 15), COMPONENTS)
    chosen = jax.vmap(lambda member_key: jax.random.permutation(member_key, PB)[:NBB])(member_keys)
    return chosen.astype(jnp.int32)


def draw_parent_modes(key, part):
    position = jnp.arange(NP, dtype=jnp.float32) / (NP - 1)
    values = jnp.clip(jax.random.normal(jax.random.fold_in(key, 16), (NP, MODES), jnp.float32), -4.0, 4.0)
    row_scale = 1.0 + 2.0 * position
    return jnp.clip(values * row_scale[:, None] / NP ** 0.5, -2.0, 2.0)


def place_ends(result, own_key, smallest, top_value):
    longest = result.shape.index(max(result.shape))
    spots = []
    for shift in (0, 1):
        where = [jax.random.randint(jax.random.fold_in(own_key, axis), (), 0, length) for axis, length in enumerate(result.shape)]
        where[longest] = (where[longest] + shift) % result.shape[longest]
        spots.append(tuple(where))
    return result.at[spots[0]].set(smallest).at[spots[1]].set(top_value)


def block_levels(rng, shape, shards, least, top_value):
    def one(axis_at, parts):
        steps = jax.random.uniform(jax.random.fold_in(jax.random.fold_in(rng, 6), axis_at), (parts,), jnp.float32, least / len(shards), top_value / len(shards))
        return jnp.repeat(jnp.exp(steps), shape[axis_at] // parts).reshape((-1,) + (1,) * (len(shape) - axis_at - 1))

    gain = one(*shards[0])
    for cut in shards[1:]:
        gain = gain * one(*cut)
    return gain


def scatter_about(key, dims, deviation, reach, pieces=(), kind=jnp.bfloat16):
    values = deviation * jax.random.normal(key, dims, jnp.float32)
    if pieces:
        values = values * block_levels(key, dims, pieces, -0.22, 0.18)
    return jnp.clip(values, -reach, reach).astype(kind)


def setup_inputs(seed: int = 0) -> dict:
    keys = jax.random.split(jax.random.key(seed), 11)
    return {
        "interior_stiffness": draw_interior_stiffness(jax.random.fold_in(keys[10], 71), 0),
        "interior_links": draw_interior_links(jax.random.fold_in(keys[10], 71), 0),
        "coupling_stiffness": scatter_about(keys[2], (COMPONENTS, BLOCK, NB), BLOCK ** -0.5, 0.5, ((0, 32),), jnp.float32),
        "interface_stiffness": draw_interface_stiffness(jax.random.fold_in(keys[10], 71), 0),
        "interior_mass": jnp.clip(jnp.exp(math.log(0.5) - 2.8134107 * jax.random.uniform(keys[4], (COMPONENTS, MAXI), jnp.float32) ** block_levels(keys[4], (COMPONENTS, MAXI), ((0, 32),), -0.2, 0.2)), 0.03, 0.5),
        "interface_mass": jnp.clip(jnp.exp(math.log(4.0) - 2.0794415 * jax.random.uniform(keys[5], (COMPONENTS, NB), jnp.float32) ** block_levels(keys[5], (COMPONENTS, NB), ((0, 32),), -0.2, 0.2)), 0.5, 4.0),
        "interior_modes": scatter_about(keys[6], (COMPONENTS, MAXI, MODES), 1.0, 6.0, ((0, 32),), jnp.float32),
        "interior_blocks": place_ends(jax.random.randint(keys[7], (COMPONENTS,), MAXB // 3, MAXB + 1), jax.random.fold_in(keys[7], 1), MAXB // 3, MAXB).astype(jnp.int32),
        "interface_blocks": draw_interface_blocks(jax.random.fold_in(keys[10], 71), 0),
        "parent_modes": draw_parent_modes(jax.random.fold_in(keys[10], 71), 0),
    }


def product(left, right):
    return jnp.dot(left.astype(jnp.float32), right.astype(jnp.float32), precision=lax.Precision.HIGHEST, preferred_element_type=jnp.float32)

def eliminate(diag_blocks, link_blocks, live_count):
    blocks_total = diag_blocks.shape[0]
    block_width = diag_blocks.shape[1]
    identity = jnp.eye(block_width, dtype=jnp.float32)
    positions = lax.iota(jnp.int32, blocks_total)
    diag_live = jnp.where((positions < live_count)[:, None, None], diag_blocks, identity)
    links_live = jnp.where((positions[1:] < live_count)[:, None, None], link_blocks, jnp.zeros_like(link_blocks))
    coupled_in = jnp.concatenate([jnp.zeros((1, block_width, block_width), jnp.float32), links_live], 0)

    def advance(previous, pair):
        block_diag, block_low = pair
        crossing = lax.linalg.triangular_solve(previous, block_low, left_side=False, lower=True, transpose_a=True)
        schur_part = block_diag - product(crossing, crossing.T)
        factor = jnp.linalg.cholesky(schur_part)
        return (factor, (factor, crossing))
    _, (factors, crossings) = lax.scan(advance, identity, (diag_live, coupled_in))
    return (factors, crossings)

def solve_constraint(factors, crossings, coupled_stiff, live_count):
    blocks_total = factors.shape[0]
    block_width = factors.shape[1]
    last_block = (live_count - 1).astype(jnp.int32)
    end_factor = lax.dynamic_index_in_dim(factors, last_block, 0, keepdims=False)
    forward = lax.linalg.triangular_solve(end_factor, coupled_stiff, left_side=True, lower=True)
    ahead_links = jnp.concatenate([crossings[1:], jnp.zeros((1, block_width, block_width), jnp.float32)], 0)
    positions = lax.iota(jnp.int32, blocks_total)

    def advance(following, triple):
        factor, cross_next, position = triple
        source = jnp.where(position == last_block, forward, jnp.zeros_like(forward))
        right_side = source - product(cross_next.T, following)
        solved = lax.linalg.triangular_solve(factor, right_side, left_side=True, lower=True, transpose_a=True)
        return (solved, solved)
    _, solved = lax.scan(advance, jnp.zeros_like(forward), (factors, ahead_links, positions), reverse=True)
    return -solved

def reduce_component(diag_blocks, link_blocks, coupled_stiff, edge_stiff, inner_mass, edge_mass, inner_modes, live_count):
    blocks_total = diag_blocks.shape[0]
    block_width = diag_blocks.shape[1]
    factors, crossings = eliminate(diag_blocks, link_blocks, live_count)
    constraint = solve_constraint(factors, crossings, coupled_stiff, live_count)
    end_rows = lax.dynamic_index_in_dim(constraint, (live_count - 1).astype(jnp.int32), 0, keepdims=False)
    reduced_stiff = edge_stiff + product(coupled_stiff.T, end_rows)
    live_rows = (lax.iota(jnp.int32, blocks_total * block_width) < live_count * block_width).astype(jnp.float32)
    flattened = constraint.reshape(blocks_total * block_width, constraint.shape[2])
    weighted = flattened * (inner_mass * live_rows)[:, None]
    reduced_mass = jnp.diag(edge_mass) + product(flattened.T, weighted)
    coupled_modes = product((inner_modes * live_rows[:, None]).T, weighted)
    return (reduced_stiff, reduced_mass, coupled_modes)

def place_block(accumulated, reduced, targets):
    for row_block in range(NBB):
        for col_block in range(NBB):
            row_anchor = (targets[row_block] * BLOCK).astype(jnp.int32)
            col_anchor = (targets[col_block] * BLOCK).astype(jnp.int32)
            current = lax.dynamic_slice(accumulated, (row_anchor, col_anchor), (BLOCK, BLOCK))
            addition = reduced[row_block * BLOCK:(row_block + 1) * BLOCK, col_block * BLOCK:(col_block + 1) * BLOCK]
            accumulated = lax.dynamic_update_slice(accumulated, current + addition, (row_anchor, col_anchor))
    return accumulated

def reference(interior_stiffness, interior_links, coupling_stiffness, interface_stiffness, interior_mass, interface_mass, interior_modes, interior_blocks, interface_blocks, parent_modes):

    def reduce_step(running, member):
        stiff_sum, mass_sum = running
        reduced_stiff, reduced_mass, coupled_modes = reduce_component(*member[:8])
        stiff_sum = place_block(stiff_sum, reduced_stiff, member[8])
        mass_sum = place_block(mass_sum, reduced_mass, member[8])
        return ((stiff_sum, mass_sum), coupled_modes)
    empty_sum = jnp.zeros((NP, NP), jnp.float32)
    members = (interior_stiffness, interior_links, coupling_stiffness, interface_stiffness, interior_mass, interface_mass, interior_modes, interior_blocks, interface_blocks)
    (stiff_sum, mass_sum), coupling = lax.scan(reduce_step, (empty_sum, empty_sum), members)
    scaling = (PB / (COMPONENTS * NBB)) ** 0.5
    parent_stiffness = stiff_sum * scaling
    parent_mass = mass_sum * scaling
    modal_stiffness = product(parent_modes.T, product(parent_stiffness, parent_modes))
    modal_mass = product(parent_modes.T, product(parent_mass, parent_modes))
    return (parent_stiffness, parent_mass, coupling, modal_stiffness, modal_mass)
```

```python
import functools
import jax
import jax.numpy as jnp
from jax import lax
from jax.experimental import pallas as pl
from jax.experimental.pallas import tpu as pltpu
from jax.sharding import PartitionSpec as P

AXES = ("grp", "dev")
PB = 8

PANEL = 16


def mm(left, right):
    return lax.dot_general(
        left, right, (((1,), (0,)), ((), ())),
        precision=lax.Precision.HIGHEST, preferred_element_type=jnp.float32,
    )


def sweep_panel(work, chains, width, index):
    start = index * PANEL
    rows = pl.ds(start, PANEL)
    lane = lax.broadcasted_iota(jnp.int32, (PANEL, width), 1)
    sub = lax.broadcasted_iota(jnp.int32, (PANEL, width), 0)
    chain_of = (lane // PANEL) % chains
    panels = [work[g, rows, :] for g in range(chains)]
    columns = []
    for j in range(PANEL):
        packed = None
        for g in range(chains):
            column = jnp.broadcast_to(panels[g][:, start + j : start + j + 1], (PANEL, width))
            packed = column if packed is None else jnp.where(chain_of == g, column, packed)
        columns.append(packed)
    for s in range(PANEL):
        here = columns[s]
        pivot = here[s : s + 1, :]
        inverse = 1.0 / pivot
        scaled = here * inverse
        lowered = jnp.where(sub == s, here - 1.0, here)
        for j in range(PANEL):
            if j != s:
                columns[j] = columns[j] - lowered * scaled[j : j + 1, :]
        columns[s] = jnp.where(sub == s, -inverse, scaled)
    compact = jnp.zeros((PANEL, width), jnp.float32)
    for j in range(PANEL):
        compact = jnp.where(lane % PANEL == j, columns[j], compact)
    stacked = jnp.concatenate(
        [jnp.where(lane // PANEL == g, compact, 0.0) for g in range(chains)], 0
    )
    mine = lane // PANEL == index
    unit = jnp.where(lane - start == sub, -1.0, 0.0)
    sources = [jnp.where(mine, unit, panels[g]) for g in range(chains)]
    fill = width - chains * PANEL
    if fill > 0:
        sources.append(jnp.zeros((fill, width), jnp.float32))
    reduced = mm(stacked, jnp.concatenate(sources, 0))
    mine_all = lax.broadcasted_iota(jnp.int32, (width, width), 1) // PANEL == index
    for g in range(chains):
        part = reduced[g * PANEL : (g + 1) * PANEL]
        pieces = []
        if start > 0:
            pieces.append(jnp.zeros((start, width), jnp.float32))
        pieces.append(part)
        if start + PANEL < width:
            pieces.append(jnp.zeros((width - start - PANEL, width), jnp.float32))
        weights = jnp.concatenate(pieces, 0)
        current = work[g]
        work[g] = jnp.where(mine_all, 0.0, current) + mm(current, weights)
        work[g, rows, :] = -part


def reduce_kernel(
    counts, place, diag, links, coupled, edge, inner_mass, edge_mass, modes,
    reduced_out, coupling_out, *rest,
):
    pieces_out = rest[:-6]
    work, state, moved, ahead, source, solved = rest[-6:]
    members, blocks, width, _ = diag.shape
    chains = 2 * members
    columns_total = coupled.shape[2]
    live = [counts[c] for c in range(members)]
    middle = [live[c] // 2 for c in range(members)]
    below = [live[c] - 1 - middle[c] for c in range(members)]
    levels = middle[0]
    for c in range(1, members):
        levels = jnp.maximum(levels, middle[c])
    for c in range(members):
        work[2 * c] = diag[c, 0]
        state[2 * c] = diag[c, 0]
        work[2 * c + 1] = diag[c, live[c] - 1]
        state[2 * c + 1] = diag[c, live[c] - 1]
        source[c] = coupled[c]
        solved[c] = jnp.zeros(solved.shape[1:], jnp.float32)

    def level(t, carry):
        for index in range(width // PANEL):
            sweep_panel(work, chains, width, index)

        @pl.when(t < levels)
        def _():
            for c in range(members):
                top = jnp.minimum(t, blocks - 2)
                top_after = jnp.minimum(t + 1, blocks - 1)
                bottom = jnp.maximum(live[c] - 2 - t, 0)
                link_top = links[c, top]
                link_bottom = links[c, bottom]
                moved_top = mm(work[2 * c], link_top.T)
                moved_bottom = mm(work[2 * c + 1], link_bottom)
                moved[t, 2 * c] = moved_top
                moved[t, 2 * c + 1] = moved_bottom
                moved_t = moved_bottom.T
                ahead[t, c] = mm(work[2 * c + 1], source[c])
                next_top = diag[c, top_after] + mm(link_top, moved_top)
                next_bottom = diag[c, bottom] + mm(moved_t, link_bottom)
                next_source = mm(moved_t, source[c])
                next_top = jnp.where(t < middle[c], next_top, state[2 * c])
                next_bottom = jnp.where(t < below[c], next_bottom, state[2 * c + 1])
                source[c] = jnp.where(t < below[c], next_source, source[c])
                state[2 * c] = next_top
                state[2 * c + 1] = next_bottom
                joined = next_top - (diag[c, middle[c]] - next_bottom)
                last = t == levels - 1
                work[2 * c] = jnp.where(last, joined, next_top)
                work[2 * c + 1] = jnp.where(last, joined, next_bottom)

        return carry

    lax.fori_loop(0, levels + 1, level, 0)
    for c in range(members):
        solved[c, middle[c]] = mm(work[2 * c], source[c])

    def back(s, carry):
        for c in range(members):
            top = middle[c] - 1 - s
            top_live = top >= 0
            top_safe = jnp.maximum(top, 0)
            upper = mm(moved[top_safe, 2 * c], solved[c, top_safe + 1])
            bottom = middle[c] + 1 + s
            bottom_live = bottom < live[c]
            bottom_safe = jnp.where(bottom_live, bottom, 1)
            step = jnp.where(bottom_live, live[c] - 1 - bottom, 0)
            lower = ahead[step, c] + mm(moved[step, 2 * c + 1], solved[c, bottom_safe - 1])
            solved[c, jnp.where(top_live, top, blocks)] = upper
            solved[c, jnp.where(bottom_live, bottom, blocks)] = lower
        return carry

    lax.fori_loop(0, levels, back, 0)
    row = lax.broadcasted_iota(jnp.int32, (columns_total, columns_total), 0)
    column = lax.broadcasted_iota(jnp.int32, (columns_total, columns_total), 1)
    for c in range(members):
        reduced_out[c, 0] = edge[c] + mm(coupled[c].T, solved[c, live[c] - 1])
        flat = solved[c, :blocks].reshape(blocks * width, columns_total)
        inside = lax.broadcasted_iota(jnp.int32, (1, blocks * width), 1) < live[c] * width
        weight = jnp.where(inside, inner_mass[c : c + 1, :], 0.0)
        heavy = flat.T * weight
        diagonal = jnp.where(row == column, edge_mass[c : c + 1, :], 0.0)
        reduced_out[c, 1] = diagonal + mm(heavy, flat)
        coupling_out[c] = mm(jnp.where(inside, modes[c].T, 0.0) * weight, flat)


    parts = len(pieces_out)
    owned = width // parts
    for m in range(parts):
        begin = pl.multiple_of((place[0] ^ m) * owned, owned)
        for c in range(members):
            for kind in range(2):
                for a in range(columns_total // width):
                    pieces_out[m][c, kind, a] = reduced_out[
                        c, kind, pl.ds(a * width + begin, owned), :
                    ]


def reduce_members(counts, place, parts, diag, links, coupled, edge, inner_mass, edge_mass, modes):
    members, blocks, width, _ = diag.shape
    columns_total = coupled.shape[2]
    modes_total = modes.shape[2]
    depth = blocks // 2
    owned = width // parts
    vmem = pl.BlockSpec(memory_space=pltpu.VMEM)
    smem = pl.BlockSpec(memory_space=pltpu.SMEM)
    f32 = jnp.float32
    piece = jax.ShapeDtypeStruct((members, 2, columns_total // width, owned, columns_total), f32)
    return pl.pallas_call(
        reduce_kernel,
        out_shape=(
            jax.ShapeDtypeStruct((members, 2, columns_total, columns_total), f32),
            jax.ShapeDtypeStruct((members, modes_total, columns_total), f32),
        )
        + (piece,) * parts,
        in_specs=[smem, smem] + [vmem] * 7,
        out_specs=(vmem,) * (2 + parts),
        scratch_shapes=[
            pltpu.VMEM((2 * members, width, width), f32),
            pltpu.VMEM((2 * members, width, width), f32),
            pltpu.VMEM((depth, 2 * members, width, width), f32),
            pltpu.VMEM((depth, members, width, columns_total), f32),
            pltpu.VMEM((members, width, columns_total), f32),
            pltpu.VMEM((members, blocks + 1, width, columns_total), f32),
        ],
        cost_estimate=pl.CostEstimate(
            flops=20_000_000_000, bytes_accessed=8_000_000, transcendentals=0
        ),
        name="reduce_members",
    )(counts, place, diag, links, coupled, edge, inner_mass, edge_mass, modes)


def modal_kernel(targets, reduced, modes, local_out):
    members, kinds, columns_total, _ = reduced.shape
    edges = targets.shape[0] // members
    width = columns_total // edges
    for kind in range(kinds):
        total = None
        for c in range(members):
            picked = jnp.concatenate(
                [
                    modes[pl.ds(pl.multiple_of(targets[c * edges + a] * width, width), width), :]
                    for a in range(edges)
                ],
                0,
            )
            part = mm(picked.T, mm(reduced[c, kind], picked))
            total = part if total is None else total + part
        local_out[kind] = total


def modal_share(targets, reduced, modes):
    vmem = pl.BlockSpec(memory_space=pltpu.VMEM)
    width = modes.shape[1]
    return pl.pallas_call(
        modal_kernel,
        out_shape=jax.ShapeDtypeStruct((reduced.shape[1], width, width), jnp.float32),
        in_specs=[pl.BlockSpec(memory_space=pltpu.SMEM), vmem, vmem],
        out_specs=vmem,
        cost_estimate=pl.CostEstimate(
            flops=1_000_000_000, bytes_accessed=2_000_000, transcendentals=0
        ),
        name="modal_share",
    )(targets, reduced, modes)


def gather_kernel(stride, targets, bit, *refs):
    parts = len(refs) - 3
    pieces = refs[:parts]
    keep_out, send_out, total = refs[parts:]
    slots = total.shape[0]
    members, kinds, edges, owned, columns_total = pieces[0].shape
    width = columns_total // edges
    total[...] = jnp.zeros_like(total)
    for m in range(parts):
        for c in range(members):
            where = [targets[(m * members + c) * edges + a] for a in range(edges)]
            for kind in range(kinds):
                for a in range(edges):
                    for b in range(edges):
                        at = pl.ds(pl.multiple_of(where[b] * width, width), width)
                        total[where[a], kind, :, at] += pieces[m][
                            c, kind, a, :, b * width : (b + 1) * width
                        ]
    mine = bit[0]
    for slot in range(slots // 2):
        first = (slot // stride) * 2 * stride + slot % stride
        keep_out[slot] = total[first + mine * stride]
        send_out[slot] = total[first + (1 - mine) * stride]


def gather_rows(targets, bit, stride, pieces, slots):
    members, kinds, edges, owned, columns_total = pieces[0].shape
    full = slots * (columns_total // edges)
    vmem = pl.BlockSpec(memory_space=pltpu.VMEM)
    smem = pl.BlockSpec(memory_space=pltpu.SMEM)
    half = jax.ShapeDtypeStruct((slots // 2, kinds, owned, full), jnp.float32)
    return pl.pallas_call(
        functools.partial(gather_kernel, stride),
        out_shape=(half, half),
        in_specs=[smem, smem] + [vmem] * len(pieces),
        out_specs=(vmem, vmem),
        scratch_shapes=[pltpu.VMEM((slots, kinds, owned, full), jnp.float32)],
        cost_estimate=pl.CostEstimate(
            flops=100_000_000, bytes_accessed=4_000_000, transcendentals=0
        ),
        name="gather_rows",
    )(targets, bit, *pieces)


def on_device(
    interior_stiffness,
    interior_links,
    coupling_stiffness,
    interface_stiffness,
    interior_mass,
    interface_mass,
    interior_modes,
    interior_blocks,
    interface_blocks,
    parent_modes,
):
    cores = lax.axis_size("dev")
    devices = lax.axis_size("grp") * cores
    members, edges = interface_blocks.shape
    per_block = devices // PB
    me = lax.axis_index(AXES)

    def across(value, mask):
        return lax.ppermute(value, AXES, [(d, d ^ mask) for d in range(devices)])

    spread_modes = jnp.broadcast_to(parent_modes[None], (devices,) + parent_modes.shape)
    all_modes = lax.all_to_all(spread_modes, AXES, 0, 0, tiled=True).reshape(
        devices * parent_modes.shape[0], parent_modes.shape[1]
    )
    targets = [interface_blocks.reshape(-1)]
    for m in range(1, per_block):
        targets.append(across(targets[0], m))
    reduced, coupling, *pieces = reduce_members(
        interior_blocks,
        (me % per_block)[None],
        per_block,
        interior_stiffness,
        interior_links,
        coupling_stiffness,
        interface_stiffness,
        interior_mass,
        interface_mass,
        interior_modes,
    )
    arrived = [pieces[0]] + [across(pieces[m], m) for m in range(1, per_block)]
    share = modal_share(targets[0], reduced, all_modes)
    kinds, modes_total, _ = share.shape
    rows = modes_total // devices
    split = share.reshape(kinds, devices, rows, modes_total).transpose(1, 0, 2, 3)
    modal_in = lax.all_to_all(split, AXES, 0, 0, tiled=True)
    modal_rows = modal_in.reshape(devices, kinds, rows, modes_total).sum(0)
    scaling = (PB / (members * devices * edges)) ** 0.5
    modal_rows = modal_rows * scaling
    modal_all = lax.all_to_all(
        jnp.broadcast_to(modal_rows[None], (devices,) + modal_rows.shape), AXES, 0, 0, tiled=True
    )
    modal = modal_all.transpose(1, 0, 2, 3).reshape(kinds, modes_total, modes_total)

    strides = [per_block << k for k in range(PB.bit_length() - 1)]
    order = sorted(strides, key=lambda stride: (stride != cores, -stride))
    bits = {stride: (me // stride) % 2 for stride in strides}
    first = order[0]
    keep, send = gather_rows(
        jnp.concatenate(targets), bits[first][None], first // per_block, arrived, PB
    )
    remaining = sorted(strides, reverse=True)
    remaining.remove(first)
    tail = keep.shape[1:]
    keep = keep.reshape((2,) * len(remaining) + tail)
    got = across(send, first).reshape(keep.shape)
    for stride in order[1:]:
        axis = remaining.index(stride)
        remaining.remove(stride)
        bit = bits[stride]

        def pick(which):
            return lax.dynamic_index_in_dim(keep, which, axis, False) + lax.dynamic_index_in_dim(
                got, which, axis, False
            )

        send = pick(1 - bit)
        got_next = across(send, stride)
        keep, got = pick(bit), got_next
    total = (keep + got) * scaling
    return (total[0], total[1], coupling, modal[0], modal[1])


def solution(mesh):
    placed = (
        P(AXES, None, None, None),
        P(AXES, None, None, None),
        P(AXES, None, None),
        P(AXES, None, None),
        P(AXES, None),
        P(AXES, None),
        P(AXES, None, None),
        P(AXES),
        P(AXES, None),
        P(AXES, None),
    )
    return jax.shard_map(
        on_device,
        mesh=mesh,
        in_specs=placed,
        out_specs=(P(AXES, None), P(AXES, None), P(AXES, None, None), P(), P()),
        check_vma=False,
    )
```

```python
import functools
import jax
import jax.numpy as jnp
from jax import lax
from jax.experimental import pallas as pl
from jax.experimental.pallas import tpu as pltpu
from jax.sharding import PartitionSpec as P


AXES = ("grp", "dev")
PB = 8

PANEL = 16


def dot(left, right):
    return lax.dot_general(
        left, right, (((1,), (0,)), ((), ())), preferred_element_type=jnp.float32
    )


def mm_high(left, right):
    return lax.dot_general(
        left, right, (((1,), (0,)), ((), ())),
        precision=lax.Precision.HIGH, preferred_element_type=jnp.float32,
    )


def split(value):
    high = value.astype(jnp.bfloat16)
    rest = value - high.astype(jnp.float32)
    middle = rest.astype(jnp.bfloat16)
    low = (rest - middle.astype(jnp.float32)).astype(jnp.bfloat16)
    return high, middle, low


def mm(left, right):
    columns = right.shape[1]
    left_high, left_middle, left_low = split(left)
    high, middle, low = split(right)
    near = jnp.concatenate([left_high, left_middle], 1)
    far = jnp.concatenate([left_high, left_low], 1)
    small = dot(far, jnp.concatenate([low, high], 0))
    if columns <= left.shape[1]:
        both = dot(near, jnp.concatenate([jnp.concatenate([high, middle], 1)] * 2, 0))
        return (small + both[:, columns:]) + both[:, :columns]
    return (small + dot(near, jnp.concatenate([middle] * 2, 0))) + dot(
        near, jnp.concatenate([high] * 2, 0)
    )


def sweep(work, chains, width):
    total = width // PANEL
    panels = [work[g, pl.ds(0, PANEL), :] for g in range(chains)]
    for index in range(total):
        panels = sweep_panel(work, panels, chains, width, index)


def sweep_panel(work, panels, chains, width, index):
    start = index * PANEL
    lane = lax.broadcasted_iota(jnp.int32, (PANEL, width), 1)
    sub = lax.broadcasted_iota(jnp.int32, (PANEL, width), 0)
    chain_of = (lane // PANEL) % chains
    columns = []
    for j in range(PANEL):
        packed = None
        for g in range(chains):
            column = jnp.broadcast_to(panels[g][:, start + j : start + j + 1], (PANEL, width))
            packed = column if packed is None else jnp.where(chain_of == g, column, packed)
        columns.append(packed)
    turned = []
    weights_high, weights_middle, weights_low = [], [], []
    mine = lane // PANEL == index
    unit = jnp.where(lane - start == sub, -1.0, 0.0)
    for g in range(chains):
        high, middle, low = split(panels[g])
        turned.append(jnp.concatenate([high, high, high, middle, middle, low], 0).T)
        high, middle, low = split(jnp.where(mine, unit, panels[g]))
        weights_high.append(high)
        weights_middle.append(middle)
        weights_low.append(low)
    for s in range(PANEL):
        here = columns[s]
        inverse = 1.0 / here[s : s + 1, :]
        scaled = here * inverse
        lowered = jnp.where(sub == s, here - 1.0, here)
        for j in range(PANEL):
            if j != s:
                columns[j] = columns[j] - lowered * scaled[j : j + 1, :]
        columns[s] = jnp.where(sub == s, -inverse, scaled)
    compact = columns[0]
    for j in range(1, PANEL):
        compact = jnp.where(lane % PANEL == j, columns[j], compact)
    group = lane // PANEL
    front = lane < chains * PANEL
    high, middle, low = split(compact)
    high, middle, low = (part.astype(jnp.float32) for part in (high, middle, low))
    front_back = [jnp.where(front, high, middle), jnp.where(front, low, high)]
    stacked = [
        jnp.concatenate(
            [
                jnp.where((group % chains == g) & (group < 2 * chains), part, 0.0)
                for g in range(chains)
            ],
            0,
        ).astype(jnp.bfloat16)
        for part in front_back
    ]
    fill = width - 2 * chains * PANEL
    blank = [jnp.zeros((fill, width), jnp.bfloat16)] if fill > 0 else []
    reduced = dot(stacked[1], jnp.concatenate(weights_high + weights_low + blank, 0))
    reduced = reduced + dot(stacked[0], jnp.concatenate(weights_middle * 2 + blank, 0))
    reduced = reduced + dot(stacked[0], jnp.concatenate(weights_high * 2 + blank, 0))
    after = start + PANEL
    last = after == width
    parts = [reduced[g * PANEL : (g + 1) * PANEL] for g in range(chains)]
    stacks = []
    for g in range(chains):
        high, middle, low = split(parts[g])
        stacks.append(jnp.concatenate([high, middle, low, high, middle, high], 0))
    following = []
    if not last:
        for g in range(chains):
            change = dot(turned[g][after : after + PANEL], stacks[g])
            kept = jnp.where(mine, 0.0, work[g, pl.ds(after, PANEL), :])
            following.append(kept + change)
    for g in range(chains):
        if start > 0:
            here = jnp.where(
                lax.broadcasted_iota(jnp.int32, (start, width), 1) // PANEL == index,
                0.0,
                work[g, :start, :],
            )
            work[g, :start, :] = here + dot(turned[g][:start], stacks[g])
        rest = after + PANEL
        if rest < width:
            here = jnp.where(
                lax.broadcasted_iota(jnp.int32, (width - rest, width), 1) // PANEL == index,
                0.0,
                work[g, rest:, :],
            )
            work[g, rest:, :] = here + dot(turned[g][rest:], stacks[g])
        work[g, pl.ds(start, PANEL), :] = -parts[g]
    return following


def reduce_kernel(
    counts, place, diag, links, coupled, edge, inner_mass, edge_mass, modes,
    reduced_out, coupling_out, *rest,
):
    pieces_out = rest[:-6]
    work, state, moved, ahead, source, solved = rest[-6:]
    members, blocks, width, _ = diag.shape
    chains = 2 * members
    columns_total = coupled.shape[2]
    live = [counts[c] for c in range(members)]
    middle = [live[c] // 2 for c in range(members)]
    below = [live[c] - 1 - middle[c] for c in range(members)]
    levels = middle[0]
    for c in range(1, members):
        levels = jnp.maximum(levels, middle[c])
    for c in range(members):
        work[2 * c] = diag[c, 0]
        state[2 * c] = diag[c, 0]
        work[2 * c + 1] = diag[c, live[c] - 1]
        state[2 * c + 1] = diag[c, live[c] - 1]
        source[c] = coupled[c]
        solved[c] = jnp.zeros(solved.shape[1:], jnp.float32)

    def level(t, carry):
        sweep(work, chains, width)
        last = t == levels - 1
        for c in range(members):
            top = jnp.minimum(t, blocks - 2)
            top_after = jnp.minimum(t + 1, blocks - 1)
            bottom = jnp.maximum(live[c] - 2 - t, 0)
            link_top = links[c, top]
            link_bottom = links[c, bottom]
            top_work, bottom_work = work[2 * c], work[2 * c + 1]
            moved_top = mm(top_work, link_top.T)
            moved_bottom = mm(bottom_work, link_bottom)
            ahead_now = mm(bottom_work, source[c])
            moved[t, 2 * c] = moved_top
            moved[t, 2 * c + 1] = moved_bottom
            ahead[t, c] = ahead_now
            link_turned = link_bottom.T
            next_top = diag[c, top_after] + mm(link_top, moved_top)
            next_bottom = diag[c, bottom] + mm(link_turned, moved_bottom)
            next_source = mm(link_turned, ahead_now)
            next_top = jnp.where(t < middle[c], next_top, state[2 * c])
            next_bottom = jnp.where(t < below[c], next_bottom, state[2 * c + 1])
            source[c] = jnp.where(t < below[c], next_source, source[c])
            state[2 * c] = next_top
            state[2 * c + 1] = next_bottom
            work[2 * c] = next_top
            work[2 * c + 1] = next_bottom

        @pl.when(last)
        def _():
            for c in range(members):
                joined = state[2 * c] - (diag[c, middle[c]] - state[2 * c + 1])
                work[c] = joined

        return carry

    lax.fori_loop(0, levels, level, 0)
    sweep(work, members, width)
    for c in range(members):
        solved[c, middle[c]] = mm(work[c], source[c])

    def back(s, carry):
        for c in range(members):
            top = middle[c] - 1 - s
            top_live = top >= 0
            top_safe = jnp.maximum(top, 0)
            upper = mm(moved[top_safe, 2 * c], solved[c, top_safe + 1])
            bottom = middle[c] + 1 + s
            bottom_live = bottom < live[c]
            bottom_safe = jnp.where(bottom_live, bottom, 1)
            step = jnp.where(bottom_live, live[c] - 1 - bottom, 0)
            lower = ahead[step, c] + mm(moved[step, 2 * c + 1], solved[c, bottom_safe - 1])
            solved[c, jnp.where(top_live, top, blocks)] = upper
            solved[c, jnp.where(bottom_live, bottom, blocks)] = lower
        return carry

    lax.fori_loop(0, levels, back, 0)
    row = lax.broadcasted_iota(jnp.int32, (columns_total, columns_total), 0)
    column = lax.broadcasted_iota(jnp.int32, (columns_total, columns_total), 1)
    for c in range(members):
        reduced_out[c, 0] = edge[c] + mm_high(coupled[c].T, solved[c, live[c] - 1])
        flat = solved[c, :blocks].reshape(blocks * width, columns_total)
        inside = lax.broadcasted_iota(jnp.int32, (1, blocks * width), 1) < live[c] * width
        weight = jnp.where(inside, inner_mass[c : c + 1, :], 0.0)
        heavy = flat.T * weight
        diagonal = jnp.where(row == column, edge_mass[c : c + 1, :], 0.0)
        reduced_out[c, 1] = diagonal + mm_high(heavy, flat)
        coupling_out[c] = mm_high(jnp.where(inside, modes[c].T, 0.0) * weight, flat)


    parts = len(pieces_out)
    owned = width // parts
    for m in range(parts):
        begin = pl.multiple_of((place[0] ^ m) * owned, owned)
        for c in range(members):
            for kind in range(2):
                for a in range(columns_total // width):
                    pieces_out[m][c, kind, a] = reduced_out[
                        c, kind, pl.ds(a * width + begin, owned), :
                    ]


def reduce_members(counts, place, parts, diag, links, coupled, edge, inner_mass, edge_mass, modes):
    members, blocks, width, _ = diag.shape
    columns_total = coupled.shape[2]
    modes_total = modes.shape[2]
    depth = blocks // 2
    owned = width // parts
    vmem = pl.BlockSpec(memory_space=pltpu.VMEM)
    smem = pl.BlockSpec(memory_space=pltpu.SMEM)
    f32 = jnp.float32
    piece = jax.ShapeDtypeStruct((members, 2, columns_total // width, owned, columns_total), f32)
    return pl.pallas_call(
        reduce_kernel,
        out_shape=(
            jax.ShapeDtypeStruct((members, 2, columns_total, columns_total), f32),
            jax.ShapeDtypeStruct((members, modes_total, columns_total), f32),
        )
        + (piece,) * parts,
        in_specs=[smem, smem] + [vmem] * 7,
        out_specs=(vmem,) * (2 + parts),
        scratch_shapes=[
            pltpu.VMEM((2 * members, width, width), f32),
            pltpu.VMEM((2 * members, width, width), f32),
            pltpu.VMEM((depth, 2 * members, width, width), f32),
            pltpu.VMEM((depth, members, width, columns_total), f32),
            pltpu.VMEM((members, width, columns_total), f32),
            pltpu.VMEM((members, blocks + 1, width, columns_total), f32),
        ],
        cost_estimate=pl.CostEstimate(
            flops=20_000_000_000, bytes_accessed=8_000_000, transcendentals=0
        ),
        compiler_params=pltpu.CompilerParams(vmem_limit_bytes=24 * 1024 * 1024),
        name="reduce_members",
    )(counts, place, diag, links, coupled, edge, inner_mass, edge_mass, modes)


def spread_kernel(targets, modes, out):
    devices, rows, width = out.shape
    owned = modes.shape[0]
    lane = lax.broadcasted_iota(jnp.int32, (rows - owned, width), 1)
    named = jnp.zeros((rows - owned, width), jnp.int32)
    members, edges = targets.shape
    for k in range(members * edges):
        named = jnp.where(lane == k, targets[k // edges, k % edges], named)
    whole = jnp.concatenate([modes[...], named.astype(jnp.float32)], 0)
    for d in range(devices):
        out[d] = whole


def spread_modes(targets, modes, devices):
    vmem = pl.BlockSpec(memory_space=pltpu.VMEM)
    owned, width = modes.shape
    return pl.pallas_call(
        spread_kernel,
        out_shape=jax.ShapeDtypeStruct((devices, owned + 8, width), jnp.float32),
        in_specs=[pl.BlockSpec(memory_space=pltpu.SMEM), vmem],
        out_specs=vmem,
        name="spread_modes",
    )(targets, modes)


def modal_kernel(targets, reduced, modes, local_out):
    members, kinds, columns_total, _ = reduced.shape
    edges = targets.shape[1]
    parts = modes.shape[0] // PB
    owned = columns_total // edges // parts
    totals = [None] * kinds
    for c in range(members):
        picked = jnp.concatenate(
            [
                modes[targets[c, a] * parts + part, :owned, :]
                for a in range(edges)
                for part in range(parts)
            ],
            0,
        )
        turned = picked.T
        for kind in range(kinds):
            share = mm_high(turned, mm_high(reduced[c, kind], picked))
            totals[kind] = share if totals[kind] is None else totals[kind] + share
    for kind in range(kinds):
        local_out[kind] = totals[kind]


def modal_share(targets, reduced, modes):
    vmem = pl.BlockSpec(memory_space=pltpu.VMEM)
    width = modes.shape[2]
    return pl.pallas_call(
        modal_kernel,
        out_shape=jax.ShapeDtypeStruct((reduced.shape[1], width, width), jnp.float32),
        in_specs=[pl.BlockSpec(memory_space=pltpu.SMEM), vmem, vmem],
        out_specs=vmem,
        cost_estimate=pl.CostEstimate(
            flops=1_000_000_000, bytes_accessed=2_000_000, transcendentals=0
        ),
        name="modal_share",
    )(targets, reduced, modes)


def gather_kernel(stride, targets, bit, *refs):
    parts = len(refs) - 4
    pieces = refs[:parts]
    keep_out, send_out, total = refs[parts + 1 :]
    slots = total.shape[0]
    members, kinds, edges, _, columns_total = pieces[0].shape
    width = columns_total // edges
    total[...] = jnp.zeros_like(total)
    for m in range(parts):
        for c in range(members):
            where = [targets[(m * members + c) * edges + a] for a in range(edges)]
            for kind in range(kinds):
                for a in range(edges):
                    for b in range(edges):
                        at = pl.ds(pl.multiple_of(where[b] * width, width), width)
                        total[where[a], kind, :, at] += pieces[m][
                            c, kind, a, :, b * width : (b + 1) * width
                        ]
    mine = bit[0]
    for slot in range(slots // 2):
        first = (slot // stride) * 2 * stride + slot % stride
        keep_out[slot] = total[first + mine * stride]
        send_out[slot] = total[first + (1 - mine) * stride]


def gather_rows(targets, bit, stride, pieces, slots, after):
    _, kinds, edges, owned, columns_total = pieces[0].shape
    full = slots * (columns_total // edges)
    vmem = pl.BlockSpec(memory_space=pltpu.VMEM)
    smem = pl.BlockSpec(memory_space=pltpu.SMEM)
    half = jax.ShapeDtypeStruct((slots // 2, kinds, owned, full), jnp.float32)
    return pl.pallas_call(
        functools.partial(gather_kernel, stride),
        out_shape=(half, half),
        in_specs=[smem, smem] + [vmem] * len(pieces) + [pl.BlockSpec(memory_space=pl.ANY)],
        out_specs=(vmem, vmem),
        scratch_shapes=[pltpu.VMEM((slots, kinds, owned, full), jnp.float32)],
        cost_estimate=pl.CostEstimate(
            flops=100_000_000, bytes_accessed=4_000_000, transcendentals=0
        ),
        name="gather_rows",
    )(targets, bit, *pieces, after)


def on_device(
    interior_stiffness,
    interior_links,
    coupling_stiffness,
    interface_stiffness,
    interior_mass,
    interface_mass,
    interior_modes,
    interior_blocks,
    interface_blocks,
    parent_modes,
):
    cores = lax.axis_size("dev")
    devices = lax.axis_size("grp") * cores
    members, edges = interface_blocks.shape
    per_block = devices // PB
    me = lax.axis_index(AXES)

    def across(value, mask):
        return lax.ppermute(value, AXES, [(d, d ^ mask) for d in range(devices)])

    all_modes = lax.all_to_all(
        spread_modes(interface_blocks, parent_modes, devices),
        AXES, 0, 0, tiled=True,
    )
    reduced, coupling, *pieces = reduce_members(
        interior_blocks,
        (me % per_block)[None],
        per_block,
        interior_stiffness,
        interior_links,
        coupling_stiffness,
        interface_stiffness,
        interior_mass,
        interface_mass,
        interior_modes,
    )
    arrived = [pieces[0]] + [across(pieces[m], m) for m in range(1, per_block)]
    names = all_modes[:, parent_modes.shape[0], : members * edges].reshape(
        PB, per_block, members * edges
    )
    near = [
        lax.dynamic_slice(
            names, (me // per_block, (me % per_block) ^ m, 0), (1, 1, members * edges)
        ).reshape(-1)
        for m in range(per_block)
    ]
    targets = jnp.concatenate(near).astype(jnp.int32)
    scaling = (PB / (members * devices * edges)) ** 0.5
    core = (me // cores) % 2
    sides = [[d for d in range(devices) if (d // cores) % 2 == side] for side in range(2)]
    share = modal_share(interface_blocks, reduced, all_modes)
    ours = lax.dynamic_index_in_dim(share, core, 0, False)
    theirs = lax.dynamic_index_in_dim(share, 1 - core, 0, False)
    theirs = across(theirs, cores)
    ours = ours + theirs
    modes_total = ours.shape[1]
    modal_in = lax.all_to_all(
        ours.reshape(devices // 2, 2 * modes_total // devices, modes_total),
        AXES, 0, 0, tiled=True, axis_index_groups=sides,
    )
    modal_rows = modal_in.sum(0) * scaling
    modal_all = lax.all_to_all(
        jnp.broadcast_to(modal_rows[None], (devices // 2,) + modal_rows.shape),
        AXES, 0, 0, tiled=True, axis_index_groups=sides,
    ).reshape(modes_total, modes_total)
    modal_other = across(modal_all, cores)
    modal_stiffness = jnp.where(core == 0, modal_all, modal_other)
    modal_mass = jnp.where(core == 0, modal_other, modal_all)

    strides = [per_block << k for k in range(PB.bit_length() - 1)]
    first = cores
    remaining = sorted(strides, reverse=True)
    remaining.remove(first)
    bits = {stride: (me // stride) % 2 for stride in strides}
    keep, send = gather_rows(
        targets, bits[first][None], first // per_block, arrived, PB, share
    )
    tail = keep.shape[1:]
    got = across(send, first)
    shape = (2,) * len(remaining) + tail
    keep, got = keep.reshape(shape), got.reshape(shape)
    results = []
    for kind in range(tail[0]):
        pair = [lax.index_in_dim(value, kind, len(remaining), False) for value in (keep, got)]
        left = list(remaining)
        order = remaining if kind % 2 == 0 else remaining[::-1]
        for stride in order:
            axis = left.index(stride)
            left.remove(stride)

            def pick(which):
                return sum(lax.dynamic_index_in_dim(value, which, axis, False) for value in pair)

            received = across(pick(1 - bits[stride]), stride)
            pair = [pick(bits[stride]), received]
        results.append(sum(pair) * scaling)
    return (results[0], results[1], coupling, modal_stiffness, modal_mass)


def solution(mesh):
    placed = (
        P(AXES, None, None, None),
        P(AXES, None, None, None),
        P(AXES, None, None),
        P(AXES, None, None),
        P(AXES, None),
        P(AXES, None),
        P(AXES, None, None),
        P(AXES),
        P(AXES, None),
        P(AXES, None),
    )

    return jax.shard_map(
        on_device,
        mesh=mesh,
        in_specs=placed,
        out_specs=(P(AXES, None), P(AXES, None), P(AXES, None, None), P(), P()),
        check_vma=False,
    )
```

```python
import functools
import jax
import jax.numpy as jnp
from jax import lax
from jax.experimental import pallas as pl
from jax.experimental.pallas import tpu as pltpu
from jax.sharding import PartitionSpec as P


AXES = ("grp", "dev")
PB = 8

PANEL = 16


def dot(left, right):
    return lax.dot_general(
        left, right, (((1,), (0,)), ((), ())), preferred_element_type=jnp.float32
    )


def mm_high(left, right):
    return lax.dot_general(
        left, right, (((1,), (0,)), ((), ())),
        precision=lax.Precision.HIGH, preferred_element_type=jnp.float32,
    )


def split(value):
    high = value.astype(jnp.bfloat16)
    rest = value - high.astype(jnp.float32)
    middle = rest.astype(jnp.bfloat16)
    low = (rest - middle.astype(jnp.float32)).astype(jnp.bfloat16)
    return high, middle, low


def mm(left, right):
    columns = right.shape[1]
    left_high, left_middle, left_low = split(left)
    high, middle, low = split(right)
    near = jnp.concatenate([left_high, left_middle], 1)
    far = jnp.concatenate([left_high, left_low], 1)
    small = dot(far, jnp.concatenate([low, high], 0))
    if columns <= left.shape[1]:
        both = dot(near, jnp.concatenate([jnp.concatenate([high, middle], 1)] * 2, 0))
        return (small + both[:, columns:]) + both[:, :columns]
    return (small + dot(near, jnp.concatenate([middle] * 2, 0))) + dot(
        near, jnp.concatenate([high] * 2, 0)
    )


def sweep(work, chains, width):
    total = width // PANEL
    panels = [work[g, pl.ds(0, PANEL), :] for g in range(chains)]
    for index in range(total):
        panels = sweep_panel(work, panels, chains, width, index)


def sweep_panel(work, panels, chains, width, index):
    start = index * PANEL
    lane = lax.broadcasted_iota(jnp.int32, (PANEL, width), 1)
    sub = lax.broadcasted_iota(jnp.int32, (PANEL, width), 0)
    chain_of = (lane // PANEL) % chains
    columns = []
    for j in range(PANEL):
        packed = None
        for g in range(chains):
            column = jnp.broadcast_to(panels[g][:, start + j : start + j + 1], (PANEL, width))
            packed = column if packed is None else jnp.where(chain_of == g, column, packed)
        columns.append(packed)
    turned = []
    weights_high, weights_middle, weights_low = [], [], []
    mine = lane // PANEL == index
    unit = jnp.where(lane - start == sub, -1.0, 0.0)
    for g in range(chains):
        high, middle, low = split(panels[g])
        turned.append(jnp.concatenate([high, high, high, middle, middle, low], 0).T)
        high, middle, low = split(jnp.where(mine, unit, panels[g]))
        weights_high.append(high)
        weights_middle.append(middle)
        weights_low.append(low)
    for s in range(PANEL):
        here = columns[s]
        inverse = 1.0 / here[s : s + 1, :]
        scaled = here * inverse
        lowered = jnp.where(sub == s, here - 1.0, here)
        for j in range(PANEL):
            if j != s:
                columns[j] = columns[j] - lowered * scaled[j : j + 1, :]
        columns[s] = jnp.where(sub == s, -inverse, scaled)
    compact = columns[0]
    for j in range(1, PANEL):
        compact = jnp.where(lane % PANEL == j, columns[j], compact)
    group = lane // PANEL
    front = lane < chains * PANEL
    high, middle, low = split(compact)
    high, middle, low = (part.astype(jnp.float32) for part in (high, middle, low))
    front_back = [jnp.where(front, high, middle), jnp.where(front, low, high)]
    stacked = [
        jnp.concatenate(
            [
                jnp.where((group % chains == g) & (group < 2 * chains), part, 0.0)
                for g in range(chains)
            ],
            0,
        ).astype(jnp.bfloat16)
        for part in front_back
    ]
    fill = width - 2 * chains * PANEL
    blank = [jnp.zeros((fill, width), jnp.bfloat16)] if fill > 0 else []
    reduced = dot(stacked[1], jnp.concatenate(weights_high + weights_low + blank, 0))
    reduced = reduced + dot(stacked[0], jnp.concatenate(weights_middle * 2 + blank, 0))
    reduced = reduced + dot(stacked[0], jnp.concatenate(weights_high * 2 + blank, 0))
    after = start + PANEL
    last = after == width
    parts = [reduced[g * PANEL : (g + 1) * PANEL] for g in range(chains)]
    stacks = []
    for g in range(chains):
        high, middle, low = split(parts[g])
        stacks.append(jnp.concatenate([high, middle, low, high, middle, high], 0))
    following = []
    if not last:
        for g in range(chains):
            change = dot(turned[g][after : after + PANEL], stacks[g])
            kept = jnp.where(mine, 0.0, work[g, pl.ds(after, PANEL), :])
            following.append(kept + change)
    for g in range(chains):
        if start > 0:
            here = jnp.where(
                lax.broadcasted_iota(jnp.int32, (start, width), 1) // PANEL == index,
                0.0,
                work[g, :start, :],
            )
            work[g, :start, :] = here + dot(turned[g][:start], stacks[g])
        rest = after + PANEL
        if rest < width:
            here = jnp.where(
                lax.broadcasted_iota(jnp.int32, (width - rest, width), 1) // PANEL == index,
                0.0,
                work[g, rest:, :],
            )
            work[g, rest:, :] = here + dot(turned[g][rest:], stacks[g])
        work[g, pl.ds(start, PANEL), :] = -parts[g]
    return following


def reduce_kernel(
    counts, place, diag, links, coupled, edge, inner_mass, edge_mass, modes,
    reduced_out, coupling_out, *rest,
):
    pieces_out = rest[:-8]
    work, state, moved, ahead, source, solved, modes_here, modes_semaphore = rest[-8:]
    modes_copy = pltpu.make_async_copy(modes, modes_here, modes_semaphore)
    modes_copy.start()
    members, blocks, width, _ = diag.shape
    chains = 2 * members
    columns_total = coupled.shape[2]
    live = [counts[c] for c in range(members)]
    middle = [live[c] // 2 for c in range(members)]
    below = [live[c] - 1 - middle[c] for c in range(members)]
    levels = middle[0]
    for c in range(1, members):
        levels = jnp.maximum(levels, middle[c])
    for c in range(members):
        work[2 * c] = diag[c, 0]
        state[2 * c] = diag[c, 0]
        work[2 * c + 1] = diag[c, live[c] - 1]
        state[2 * c + 1] = diag[c, live[c] - 1]
        source[c] = coupled[c]
        solved[c] = jnp.zeros(solved.shape[1:], jnp.float32)

    def level(t, carry):
        sweep(work, chains, width)
        last = t == levels - 1
        for c in range(members):
            top = jnp.minimum(t, blocks - 2)
            top_after = jnp.minimum(t + 1, blocks - 1)
            bottom = jnp.maximum(live[c] - 2 - t, 0)
            link_top = links[c, top]
            link_bottom = links[c, bottom]
            top_work, bottom_work = work[2 * c], work[2 * c + 1]
            moved_top = mm(top_work, link_top.T)
            moved_bottom = mm(bottom_work, link_bottom)
            ahead_now = mm(bottom_work, source[c])
            moved[t, 2 * c] = moved_top
            moved[t, 2 * c + 1] = moved_bottom
            ahead[t, c] = ahead_now
            link_turned = link_bottom.T
            next_top = diag[c, top_after] + mm(link_top, moved_top)
            next_bottom = diag[c, bottom] + mm(link_turned, moved_bottom)
            next_source = mm(link_turned, ahead_now)
            next_top = jnp.where(t < middle[c], next_top, state[2 * c])
            next_bottom = jnp.where(t < below[c], next_bottom, state[2 * c + 1])
            source[c] = jnp.where(t < below[c], next_source, source[c])
            state[2 * c] = next_top
            state[2 * c + 1] = next_bottom
            work[2 * c] = next_top
            work[2 * c + 1] = next_bottom

        @pl.when(last)
        def _():
            for c in range(members):
                joined = state[2 * c] - (diag[c, middle[c]] - state[2 * c + 1])
                work[c] = joined

        return carry

    lax.fori_loop(0, levels, level, 0)
    sweep(work, members, width)
    for c in range(members):
        solved[c, middle[c]] = mm(work[c], source[c])

    def back(s, carry):
        for c in range(members):
            top = middle[c] - 1 - s
            top_live = top >= 0
            top_safe = jnp.maximum(top, 0)
            upper = mm(moved[top_safe, 2 * c], solved[c, top_safe + 1])
            bottom = middle[c] + 1 + s
            bottom_live = bottom < live[c]
            bottom_safe = jnp.where(bottom_live, bottom, 1)
            step = jnp.where(bottom_live, live[c] - 1 - bottom, 0)
            lower = ahead[step, c] + mm(moved[step, 2 * c + 1], solved[c, bottom_safe - 1])
            solved[c, jnp.where(top_live, top, blocks)] = upper
            solved[c, jnp.where(bottom_live, bottom, blocks)] = lower
        return carry

    lax.fori_loop(0, levels, back, 0)
    modes_copy.wait()
    row = lax.broadcasted_iota(jnp.int32, (columns_total, columns_total), 0)
    column = lax.broadcasted_iota(jnp.int32, (columns_total, columns_total), 1)
    for c in range(members):
        reduced_out[c, 0] = edge[c] + mm_high(coupled[c].T, solved[c, live[c] - 1])
        flat = solved[c, :blocks].reshape(blocks * width, columns_total)
        inside = lax.broadcasted_iota(jnp.int32, (1, blocks * width), 1) < live[c] * width
        weight = jnp.where(inside, inner_mass[c : c + 1, :], 0.0)
        heavy = flat.T * weight
        diagonal = jnp.where(row == column, edge_mass[c : c + 1, :], 0.0)
        reduced_out[c, 1] = diagonal + mm_high(heavy, flat)
        coupling_out[c] = mm_high(jnp.where(inside, modes_here[c].T, 0.0) * weight, flat)


    parts = len(pieces_out)
    owned = width // parts
    for m in range(parts):
        begin = pl.multiple_of((place[0] ^ m) * owned, owned)
        for c in range(members):
            for kind in range(2):
                for a in range(columns_total // width):
                    pieces_out[m][c, kind, a] = reduced_out[
                        c, kind, pl.ds(a * width + begin, owned), :
                    ]


def reduce_members(counts, place, parts, diag, links, coupled, edge, inner_mass, edge_mass, modes):
    members, blocks, width, _ = diag.shape
    columns_total = coupled.shape[2]
    modes_total = modes.shape[2]
    depth = blocks // 2
    owned = width // parts
    vmem = pl.BlockSpec(memory_space=pltpu.VMEM)
    smem = pl.BlockSpec(memory_space=pltpu.SMEM)
    f32 = jnp.float32
    piece = jax.ShapeDtypeStruct((members, 2, columns_total // width, owned, columns_total), f32)
    return pl.pallas_call(
        reduce_kernel,
        out_shape=(
            jax.ShapeDtypeStruct((members, 2, columns_total, columns_total), f32),
            jax.ShapeDtypeStruct((members, modes_total, columns_total), f32),
        )
        + (piece,) * parts,
        in_specs=[smem, smem] + [vmem] * 6 + [pl.BlockSpec(memory_space=pl.ANY)],
        out_specs=(vmem,) * (2 + parts),
        scratch_shapes=[
            pltpu.VMEM((2 * members, width, width), f32),
            pltpu.VMEM((2 * members, width, width), f32),
            pltpu.VMEM((depth, 2 * members, width, width), f32),
            pltpu.VMEM((depth, members, width, columns_total), f32),
            pltpu.VMEM((members, width, columns_total), f32),
            pltpu.VMEM((members, blocks + 1, width, columns_total), f32),
            pltpu.VMEM(modes.shape, f32),
            pltpu.SemaphoreType.DMA(()),
        ],
        cost_estimate=pl.CostEstimate(
            flops=20_000_000_000, bytes_accessed=8_000_000, transcendentals=0
        ),
        name="reduce_members",
    )(counts, place, diag, links, coupled, edge, inner_mass, edge_mass, modes)


def spread_kernel(targets, modes, out):
    devices, rows, width = out.shape
    owned = modes.shape[0]
    lane = lax.broadcasted_iota(jnp.int32, (rows - owned, width), 1)
    named = jnp.zeros((rows - owned, width), jnp.int32)
    members, edges = targets.shape
    for k in range(members * edges):
        named = jnp.where(lane == k, targets[k // edges, k % edges], named)
    whole = jnp.concatenate([modes[...], named.astype(jnp.float32)], 0)
    for d in range(devices):
        out[d] = whole


def spread_modes(targets, modes, devices):
    vmem = pl.BlockSpec(memory_space=pltpu.VMEM)
    owned, width = modes.shape
    return pl.pallas_call(
        spread_kernel,
        out_shape=jax.ShapeDtypeStruct((devices, owned + 8, width), jnp.float32),
        in_specs=[pl.BlockSpec(memory_space=pltpu.SMEM), vmem],
        out_specs=vmem,
        name="spread_modes",
    )(targets, modes)


def modal_kernel(targets, side, reduced, modes, ours_out, theirs_out, both):
    members, kinds, columns_total, _ = reduced.shape
    edges = targets.shape[1]
    parts = modes.shape[0] // PB
    owned = columns_total // edges // parts
    totals = [None] * kinds
    for c in range(members):
        picked = jnp.concatenate(
            [
                modes[targets[c, a] * parts + part, :owned, :]
                for a in range(edges)
                for part in range(parts)
            ],
            0,
        )
        turned = picked.T
        for kind in range(kinds):
            share = mm_high(turned, mm_high(reduced[c, kind], picked))
            totals[kind] = share if totals[kind] is None else totals[kind] + share
    for kind in range(kinds):
        both[kind] = totals[kind]
    ours_out[...] = both[side[0]]
    theirs_out[...] = both[1 - side[0]]


def modal_share(targets, side, reduced, modes):
    vmem = pl.BlockSpec(memory_space=pltpu.VMEM)
    smem = pl.BlockSpec(memory_space=pltpu.SMEM)
    width = modes.shape[2]
    return pl.pallas_call(
        modal_kernel,
        out_shape=(jax.ShapeDtypeStruct((width, width), jnp.float32),) * 2,
        in_specs=[smem, smem, vmem, vmem],
        out_specs=(vmem, vmem),
        scratch_shapes=[pltpu.VMEM((reduced.shape[1], width, width), jnp.float32)],
        cost_estimate=pl.CostEstimate(
            flops=1_000_000_000, bytes_accessed=2_000_000, transcendentals=0
        ),
        name="modal_share",
    )(targets, side, reduced, modes)


def gather_kernel(stride, targets, bit, *refs):
    parts = len(refs) - 4
    pieces = refs[:parts]
    keep_out, send_out, total = refs[parts + 1 :]
    slots = total.shape[0]
    members, kinds, edges, _, columns_total = pieces[0].shape
    width = columns_total // edges
    total[...] = jnp.zeros_like(total)
    for m in range(parts):
        for c in range(members):
            where = [targets[(m * members + c) * edges + a] for a in range(edges)]
            for kind in range(kinds):
                for a in range(edges):
                    for b in range(edges):
                        at = pl.ds(pl.multiple_of(where[b] * width, width), width)
                        total[where[a], kind, :, at] += pieces[m][
                            c, kind, a, :, b * width : (b + 1) * width
                        ]
    mine = bit[0]
    for slot in range(slots // 2):
        first = (slot // stride) * 2 * stride + slot % stride
        keep_out[slot] = total[first + mine * stride]
        send_out[slot] = total[first + (1 - mine) * stride]


def gather_rows(targets, bit, stride, pieces, slots, after):
    _, kinds, edges, owned, columns_total = pieces[0].shape
    full = slots * (columns_total // edges)
    vmem = pl.BlockSpec(memory_space=pltpu.VMEM)
    smem = pl.BlockSpec(memory_space=pltpu.SMEM)
    half = jax.ShapeDtypeStruct((slots // 2, kinds, owned, full), jnp.float32)
    return pl.pallas_call(
        functools.partial(gather_kernel, stride),
        out_shape=(half, half),
        in_specs=[smem, smem] + [vmem] * len(pieces) + [pl.BlockSpec(memory_space=pl.ANY)],
        out_specs=(vmem, vmem),
        scratch_shapes=[pltpu.VMEM((slots, kinds, owned, full), jnp.float32)],
        cost_estimate=pl.CostEstimate(
            flops=100_000_000, bytes_accessed=4_000_000, transcendentals=0
        ),
        name="gather_rows",
    )(targets, bit, *pieces, after)


def on_device(
    interior_stiffness,
    interior_links,
    coupling_stiffness,
    interface_stiffness,
    interior_mass,
    interface_mass,
    interior_modes,
    interior_blocks,
    interface_blocks,
    parent_modes,
):
    cores = lax.axis_size("dev")
    devices = lax.axis_size("grp") * cores
    members, edges = interface_blocks.shape
    per_block = devices // PB
    me = lax.axis_index(AXES)

    def across(value, mask):
        return lax.ppermute(value, AXES, [(d, d ^ mask) for d in range(devices)])

    all_modes = lax.all_to_all(
        spread_modes(interface_blocks, parent_modes, devices),
        AXES, 0, 0, tiled=True,
    )
    reduced, coupling, *pieces = reduce_members(
        interior_blocks,
        (me % per_block)[None],
        per_block,
        interior_stiffness,
        interior_links,
        coupling_stiffness,
        interface_stiffness,
        interior_mass,
        interface_mass,
        interior_modes,
    )
    arrived = [pieces[0]] + [across(pieces[m], m) for m in range(1, per_block)]
    names = all_modes[:, parent_modes.shape[0], : members * edges].reshape(
        PB, per_block, members * edges
    )
    near = [
        lax.dynamic_slice(
            names, (me // per_block, (me % per_block) ^ m, 0), (1, 1, members * edges)
        ).reshape(-1)
        for m in range(per_block)
    ]
    targets = jnp.concatenate(near).astype(jnp.int32)
    scaling = (PB / (members * devices * edges)) ** 0.5
    core = (me // cores) % 2
    sides = [[d for d in range(devices) if (d // cores) % 2 == side] for side in range(2)]
    ours, theirs = modal_share(interface_blocks, core[None], reduced, all_modes)
    theirs = across(theirs, cores)
    summed = ours + theirs
    modes_total = summed.shape[1]
    modal_in = lax.all_to_all(
        summed.reshape(devices // 2, 2 * modes_total // devices, modes_total),
        AXES, 0, 0, tiled=True, axis_index_groups=sides,
    )
    modal_rows = modal_in.sum(0) * scaling
    modal_all = lax.all_to_all(
        jnp.broadcast_to(modal_rows[None], (devices // 2,) + modal_rows.shape),
        AXES, 0, 0, tiled=True, axis_index_groups=sides,
    ).reshape(modes_total, modes_total)
    modal_other = across(modal_all, cores)
    modal_stiffness = jnp.where(core == 0, modal_all, modal_other)
    modal_mass = jnp.where(core == 0, modal_other, modal_all)

    strides = [per_block << k for k in range(PB.bit_length() - 1)]
    first = cores
    remaining = sorted(strides, reverse=True)
    remaining.remove(first)
    bits = {stride: (me // stride) % 2 for stride in strides}
    keep, send = gather_rows(
        targets, bits[first][None], first // per_block, arrived, PB, ours
    )
    tail = keep.shape[1:]
    got = across(send, first)
    shape = (2,) * len(remaining) + tail
    keep, got = keep.reshape(shape), got.reshape(shape)
    results = []
    for kind in range(tail[0]):
        pair = [lax.index_in_dim(value, kind, len(remaining), False) for value in (keep, got)]
        left = list(remaining)
        order = remaining if kind % 2 == 0 else remaining[::-1]
        for stride in order:
            axis = left.index(stride)
            left.remove(stride)

            def pick(which):
                return sum(lax.dynamic_index_in_dim(value, which, axis, False) for value in pair)

            received = across(pick(1 - bits[stride]), stride)
            pair = [pick(bits[stride]), received]
        results.append(sum(pair) * scaling)
    return (results[0], results[1], coupling, modal_stiffness, modal_mass)


def solution(mesh):
    placed = (
        P(AXES, None, None, None),
        P(AXES, None, None, None),
        P(AXES, None, None),
        P(AXES, None, None),
        P(AXES, None),
        P(AXES, None),
        P(AXES, None, None),
        P(AXES),
        P(AXES, None),
        P(AXES, None),
    )

    return jax.shard_map(
        on_device,
        mesh=mesh,
        in_specs=placed,
        out_specs=(P(AXES, None), P(AXES, None), P(AXES, None, None), P(), P()),
        check_vma=False,
    )
```
